256 devices in a mesh: pb: 16 (over y_hi, x, core), wa: 16 (over y_lo, z).
Axes of the slice: x: 4, y: 4 (y_hi: 2, y_lo: 2; y = y_hi * 2 + y_lo), z: 8, core: 2. Of those that a mesh axis runs over, the one named last changes fastest.
Arguments:
- acts: bfloat16 [4096, 28672], P('pb', 'wa'), may hold values from -6 to 6
- grads: bfloat16 [4096, 8192], P('pb', 'wa'), may hold values from -6 to 6
- query_in: bfloat16 [28672, 4096], P('wa', 'pb'), may hold values from -0.03125 to 0.03125
- query_out: bfloat16 [8192, 4096], P('wa', 'pb'), may hold values from -0.01171875 to 0.01171875
- lengths: int32 [256], replicated, may hold values from 1 to 128, 4096 in all
Outputs:
- seq_scores: float32 [128, 256], P('pb', 'wa')
The draws below stay inside these ranges and needn't reach their ends.
Inputs may be any that keep to these rules, and one draw needn't show every extreme that they name: The lengths sum to 4096 and the longest is exactly 128.
All inputs are finite; a program needn't handle non-finite values.
Results may differ from the reference program's by a relative error of at most 0.0003.
Values may be sent and summed in bfloat16 or wider, within the bound.
No kernel may reach another device: no remote copies, remote signals or barrier semaphores. Data moves between devices by JAX's collectives and lax.ppermute only.
A program may use at most 64 MiB of HBM per device.

```python
import math
import jax
import jax.numpy as jnp
import numpy as np
from jax import lax

D_IN = 28672
D_OUT = 8192
QUERIES = 128
RANK = 32
TOK_DEV = 256
TOKENS = 4096
NSEQ = 256
SEQ_MOST = 128
WINDOW = 8
N_PB = 16


def with_spikes(array, stream_key, source, target, shards_of, factor):
    owner, partner = [(jnp.arange(array.shape[axis_at]) // (array.shape[axis_at] // shards_of)).reshape([-1 if axis == axis_at else 1 for axis in range(array.ndim)]) for axis_at in (source, target)]
    chosen = jax.random.permutation(stream_key, shards_of)[partner]
    strong = (owner == chosen) | (owner == (partner + shards_of // 2) % shards_of)
    return jnp.where(strong, factor * array, array)


def levels(key, extent, split, least, largest):
    def one(axis_at, parts):
        draws = jax.random.uniform(jax.random.fold_in(jax.random.fold_in(key, 6), axis_at), (parts,), jnp.float32, least / len(split), largest / len(split))
        return jnp.repeat(jnp.exp(draws), extent[axis_at] // parts).reshape((-1,) + (1,) * (len(extent) - axis_at - 1))

    loudness = one(*split[0])
    for cut in split[1:]:
        loudness = loudness * one(*cut)
    return loudness


def profile(amount, total, reach, slope):
    loads = [(1 << 20) // math.isqrt(grade ** slope) + 1 for grade in range(2, amount + 1)]
    surplus, holding = total - reach - (amount - 1), [1] * (amount - 1)
    while surplus > 0:
        movable = [i for i in range(amount - 1) if holding[i] < reach]
        mass, remaining = sum([loads[i] for i in movable]), surplus
        for i in movable:
            extra = min(reach - holding[i], max(1, remaining * loads[i] // mass), surplus)
            holding[i] = holding[i] + extra
            surplus = surplus - extra
    return np.array([reach] + holding)


def ragged_sizes(key, number_of, total, reach, skew):
    if number_of == 2:
        one = jax.random.randint(key, (), max(1, total - reach), min(reach, total - 1) + 1)
        return jnp.stack([one, total - one])
    tallies = jnp.asarray(profile(number_of, total, reach, skew), jnp.int32)
    twos = (number_of - 1) // 2
    source_of, sink = tallies[1:1 + 2 * twos:2], tallies[2:2 + 2 * twos:2]
    slack = jnp.minimum(source_of - 1, reach - sink)
    shifted = jax.random.randint(jax.random.fold_in(key, 1), (twos,), 0, 1 << 20) % (slack + 1)
    tallies = tallies.at[1:1 + 2 * twos:2].set(source_of - shifted).at[2:2 + 2 * twos:2].set(sink + shifted)
    return tallies[jax.random.permutation(jax.random.fold_in(key, 2), number_of)]


def centred(rng, shape, width, limit, pieces=(), kind=jnp.bfloat16):
    result = jax.random.normal(rng, shape, jnp.float32) * width
    if len(pieces) > 0:
        result = levels(rng, shape, pieces, -0.22, 0.18) * result
    return jnp.clip(result, min=-limit, max=limit).astype(kind)


def heavy_noise(key, shape, deviation, most, shards, heavy, kind=jnp.bfloat16):
    values = deviation * jax.random.normal(key, shape, jnp.float32)
    if shards:
        values = values * levels(key, shape, shards, -0.22, 0.18)
    return jnp.clip(with_spikes(values, jax.random.fold_in(key, 3), *heavy), -most, most).astype(kind)


def setup_inputs(seed: int = 0) -> dict:
    splits = jax.random.split(jax.random.key(seed), 6)
    acts = heavy_noise(splits[0], (TOKENS, D_IN), 1.0, 6.0, ((0, 16), (1, 16)), (1, 0, 16, 2.0))
    grads = centred(splits[1], (TOKENS, D_OUT), 1.0, 6.0, ((0, 16), (1, 16)))
    query_in = centred(splits[2], (D_IN, QUERIES * RANK), D_IN ** -0.5, 0.03125, ((0, 16), (1, 16)))
    query_out = centred(splits[3], (D_OUT, QUERIES * RANK), (D_OUT * RANK) ** -0.5, 0.01171875, ((0, 16), (1, 16)))
    lengths = ragged_sizes(splits[4], NSEQ, TOKENS, SEQ_MOST, 2).astype(jnp.int32)
    return dict(acts=acts, grads=grads, query_in=query_in, query_out=query_out, lengths=lengths)


def reference(acts, grads, query_in, query_out, lengths):
    proj_in = jnp.dot(acts, query_in, preferred_element_type=jnp.float32)
    proj_out = jnp.dot(grads, query_out, preferred_element_type=jnp.float32)
    token_score = jnp.sum((proj_in * proj_out).reshape(TOKENS, QUERIES, RANK), axis=2)
    blocks = (lax.iota(jnp.int32, TOKENS) // TOK_DEV).astype(jnp.int32)
    qgroups = (lax.iota(jnp.int32, QUERIES) // (QUERIES // N_PB)).astype(jnp.int32)
    offset = (qgroups[None, :] - blocks[:, None] + N_PB) % N_PB
    kept = jnp.where(offset < WINDOW, token_score, jnp.zeros_like(token_score))
    ends = jnp.cumsum(lengths).astype(jnp.int32)
    starts = (ends - lengths).astype(jnp.int32)
    spots = lax.iota(jnp.int32, TOKENS)
    inside = (spots[:, None] >= starts[None, :]) & (spots[:, None] < ends[None, :])
    table = inside.astype(token_score.dtype)
    seq_total = jnp.dot(kept.T, table, precision=lax.Precision.HIGHEST)
    return seq_total / lengths.astype(token_score.dtype)[None, :]
```

```python
import jax
import jax.numpy as jnp
from jax import lax
from jax.sharding import PartitionSpec as P

RANK = 32


def moved(value, pairs):
    return lax.ppermute(value, "pb", pairs)


def project(tokens, queries):
    return jnp.dot(tokens, queries, preferred_element_type=jnp.float32)


def summed(parts, widths):
    both = jnp.concatenate(parts, axis=1)
    rows = both.shape[0] // widths
    came = lax.all_to_all(both, "wa", 0, 0, tiled=True)
    total = jnp.sum(came.reshape(widths, rows, both.shape[1]), axis=0)
    return jnp.split(total, len(parts), axis=1)


def member_table(starts, ends, first, count):
    spots = first + lax.iota(jnp.int32, count)
    inside = (spots[:, None] >= starts[None, :]) & (spots[:, None] < ends[None, :])
    return inside.astype(jnp.float32)


def query_scores(proj_in, proj_out):
    count = proj_in.shape[0]
    return jnp.sum((proj_in * proj_out).reshape(count, -1, RANK), axis=2)


def shards(acts, grads, query_in, query_out, lengths):
    groups = lax.axis_size("pb")
    widths = lax.axis_size("wa")
    group = lax.axis_index("pb")
    width_slot = lax.axis_index("wa")
    quarter, half = groups // 4, groups // 2
    tok = acts.shape[0]
    rows = tok // widths
    nseq = lengths.shape[0]
    even = group % 2 == 0

    swap = [(p, p ^ 1) for p in range(groups)]
    ahead = [(p, (p + 2) % groups) for p in range(groups)]
    back = [(p, (p - quarter) % groups) for p in range(groups)]
    flip = [(p, (p - 1 + half) % groups) for p in range(1, groups, 2)]

    side_out = moved(grads, swap)
    last_out = moved(grads, ahead)
    far_out = moved(query_out, back)
    flip_out = moved(grads, flip)
    side_in = moved(acts, swap)
    last_in = moved(acts, ahead)
    far_in = moved(query_in, back)
    flip_in = moved(acts, flip)
    lasts_out = moved(last_out, swap)
    lasts_in = moved(last_in, swap)
    edge_out = jnp.where(even, flip_out, side_out)
    edge_in = jnp.where(even, flip_in, side_in)

    in0, out0 = summed([project(acts, query_in), project(grads, query_out)], widths)
    outs = summed(
        [
            project(edge_out, query_out),
            project(last_out, query_out),
            project(lasts_out, query_out),
            project(grads, far_out),
            project(side_out, far_out),
            project(last_out, far_out),
            project(lasts_out, far_out),
        ],
        widths,
    )
    ins_a = summed(
        [
            project(edge_in, query_in),
            project(last_in, query_in),
            project(lasts_in, query_in),
        ],
        widths,
    )
    ins_b = summed(
        [
            project(acts, far_in),
            project(side_in, far_in),
            project(last_in, far_in),
            project(lasts_in, far_in),
        ],
        widths,
    )
    ends = jnp.cumsum(lengths)
    starts = ends - lengths

    def table(block):
        return member_table(starts, ends, block * tok + width_slot * rows, rows)

    own, side = group, group ^ 1
    edge = jnp.where(even, (group + groups - half + 1) % groups, side)
    last, lasts = (group + groups - 2) % groups, (side + groups - 2) % groups
    t_own, t_side, t_edge, t_last, t_lasts = [table(b) for b in (own, side, edge, last, lasts)]

    def totals(proj_in, proj_out, tables):
        scores = query_scores(jnp.concatenate(proj_in, 0), jnp.concatenate(proj_out, 0))
        return jnp.dot(scores.T, jnp.concatenate(tables, 0), precision=lax.Precision.HIGHEST)

    near_total = totals([in0, *ins_a], [out0, *outs[:3]], [t_own, t_edge, t_last, t_lasts])
    far_total = totals(ins_b, outs[3:], [t_own, t_side, t_last, t_lasts])
    share = nseq // widths
    both = jnp.concatenate([near_total, far_total], axis=0)
    both = jnp.moveaxis(both.reshape(both.shape[0], widths, share), 1, 0)
    came = jnp.sum(lax.all_to_all(both, "wa", 0, 0, tiled=True), axis=0)
    queries = near_total.shape[0]
    forward = [(p, (p + quarter) % groups) for p in range(groups)]
    mine = came[:queries] + moved(came[queries:], forward)
    lengths_float = lengths.astype(jnp.float32)
    my_lengths = lax.dynamic_slice_in_dim(lengths_float, width_slot * share, share, 0)
    return mine / my_lengths[None, :]


def solution(mesh):
    return jax.shard_map(
        shards,
        mesh=mesh,
        in_specs=(P("pb", "wa"), P("pb", "wa"), P("wa", "pb"), P("wa", "pb"), P()),
        out_specs=P("pb", "wa"),
        check_vma=False,
    )
```

```python
import jax
import jax.numpy as jnp
from jax import lax
from jax.sharding import PartitionSpec as P


RANK = 32


def moved(value, pairs):
    return lax.ppermute(value, "pb", pairs)


def project(tokens, queries):
    return jnp.dot(tokens, queries, preferred_element_type=jnp.float32)


def summed(parts, widths):
    both = jnp.concatenate(parts, axis=1)
    rows = both.shape[0] // widths
    came = lax.all_to_all(both, "wa", 0, 0, tiled=True)
    total = jnp.sum(came.reshape(widths, rows, both.shape[1]), axis=0)
    return jnp.split(total, len(parts), axis=1)


def halved(parts, widths, slot):
    both = jnp.concatenate(parts, axis=1)
    half, near = both.shape[0] // 2, widths // 2
    upper = slot // near
    given = lax.dynamic_slice_in_dim(both, (1 - upper) * half, half, 0)
    kept = lax.dynamic_slice_in_dim(both, upper * half, half, 0)
    got = lax.ppermute(given, "wa", [(w, (w + near) % widths) for w in range(widths)])
    lines = [list(range(near)), list(range(near, widths))]
    came = lax.all_to_all(kept + got, "wa", 0, 0, axis_index_groups=lines, tiled=True)
    total = jnp.sum(came.reshape(near, half // near, both.shape[1]), axis=0)
    return jnp.split(total, len(parts), axis=1)


def member_table(starts, ends, first, count):
    spots = first + lax.iota(jnp.int32, count)
    inside = (spots[:, None] >= starts[None, :]) & (spots[:, None] < ends[None, :])
    return inside.astype(jnp.float32)


def query_scores(proj_in, proj_out):
    count = proj_in.shape[0]
    return jnp.sum((proj_in * proj_out).reshape(count, -1, RANK), axis=2)


def scores(acts, grads, query_in, query_out, lengths):
    groups = lax.axis_size("pb")
    widths = lax.axis_size("wa")
    group = lax.axis_index("pb")
    width_slot = lax.axis_index("wa")
    quarter, half = groups // 4, groups // 2
    tok = acts.shape[0]
    rows = tok // widths
    nseq = lengths.shape[0]
    even = group % 2 == 0

    swap = [(p, p ^ 1) for p in range(groups)]
    ahead = [(p, (p + 2) % groups) for p in range(groups)]
    back = [(p, (p - quarter) % groups) for p in range(groups)]
    flip = [(p, (p - 1 + half) % groups) for p in range(1, groups, 2)]

    side_out = moved(grads, swap)
    last_out = moved(grads, ahead)
    far_out = moved(query_out, back)
    flip_out = moved(grads, flip)
    side_in = moved(acts, swap)
    last_in = moved(acts, ahead)
    far_in = moved(query_in, back)
    flip_in = moved(acts, flip)
    lasts_out = moved(last_out, swap)
    lasts_in = moved(last_in, swap)
    edge_out = jnp.where(even, flip_out, side_out)
    edge_in = jnp.where(even, flip_in, side_in)

    own = [project(acts, query_in), project(grads, query_out)]
    in0, out0 = summed(own, widths)
    outs = halved(
        [
            project(edge_out, query_out),
            project(last_out, query_out),
            project(lasts_out, query_out),
            project(grads, far_out),
            project(side_out, far_out),
            project(last_out, far_out),
            project(lasts_out, far_out),
        ],
        widths,
        width_slot,
    )
    ins_a = summed(
        [
            project(edge_in, query_in),
            project(last_in, query_in),
            project(lasts_in, query_in),
        ],
        widths,
    )
    ins_b = summed(
        [
            project(acts, far_in),
            project(side_in, far_in),
            project(last_in, far_in),
            project(lasts_in, far_in),
        ],
        widths,
    )
    ends = jnp.cumsum(lengths)
    starts = ends - lengths

    def table(block):
        return member_table(starts, ends, block * tok + width_slot * rows, rows)

    here, side = group, group ^ 1
    edge = jnp.where(even, (group + groups - half + 1) % groups, side)
    last, lasts = (group + groups - 2) % groups, (side + groups - 2) % groups
    t_own, t_side, t_edge, t_last, t_lasts = [table(b) for b in (here, side, edge, last, lasts)]

    def totals(proj_in, proj_out, tables):
        scores = query_scores(jnp.concatenate(proj_in, 0), jnp.concatenate(proj_out, 0))
        return jnp.dot(scores.T, jnp.concatenate(tables, 0), precision=lax.Precision.HIGHEST)

    near_total = totals([in0, *ins_a], [out0, *outs[:3]], [t_own, t_edge, t_last, t_lasts])
    far_total = totals(ins_b, outs[3:], [t_own, t_side, t_last, t_lasts])
    share = nseq // widths
    both = jnp.concatenate([near_total, far_total], axis=0)
    both = jnp.moveaxis(both.reshape(both.shape[0], widths, share), 1, 0)
    came = jnp.sum(lax.all_to_all(both, "wa", 0, 0, tiled=True), axis=0)
    queries = near_total.shape[0]
    forward = [(p, (p + quarter) % groups) for p in range(groups)]
    mine = came[:queries] + moved(came[queries:], forward)
    lengths_float = lengths.astype(jnp.float32)
    my_lengths = lax.dynamic_slice_in_dim(lengths_float, width_slot * share, share, 0)
    return mine / my_lengths[None, :]


def solution(mesh):
    return jax.shard_map(
        scores,
        mesh=mesh,
        in_specs=(P("pb", "wa"), P("pb", "wa"), P("wa", "pb"), P("wa", "pb"), P()),
        out_specs=P("pb", "wa"),
        check_vma=False,
    )
```

```python
import jax
import jax.numpy as jnp
from jax import lax
from jax.sharding import PartitionSpec as P


RANK = 32
LANES = 128


def moved(value, pairs):
    return lax.ppermute(value, "pb", pairs)


def project(tokens, queries):
    return jnp.dot(tokens, queries, preferred_element_type=jnp.float32)


def summed(parts, widths):
    both = jnp.concatenate(parts, axis=1)
    rows = both.shape[0] // widths
    came = lax.all_to_all(both, "wa", 0, 0, tiled=True)
    total = jnp.sum(came.reshape(widths, rows, both.shape[1]), axis=0)
    return jnp.split(total, len(parts), axis=1)


def summed_narrow(parts, widths):
    both = jnp.concatenate(parts, axis=1)
    rows, lanes = both.shape[0] // widths, both.shape[1]
    largest = jnp.maximum(jnp.max(jnp.abs(both)), 1e-30)
    power = 13.0 - jnp.ceil(jnp.log2(largest))
    sent = (both * jnp.exp2(power)).astype(jnp.float16)
    tag = jnp.full((both.shape[0], LANES), power, jnp.float16)
    came = lax.all_to_all(jnp.concatenate([sent, tag], axis=1), "wa", 0, 0, tiled=True)
    came = came.reshape(widths, rows, lanes + LANES).astype(jnp.float32)
    undo = jnp.exp2(-came[:, :, lanes : lanes + 1])
    total = jnp.sum(came[:, :, :lanes] * undo, axis=0)
    return jnp.split(total, len(parts), axis=1)


def member_table(starts, ends, first, count):
    spots = first + lax.iota(jnp.int32, count)
    inside = (spots[:, None] >= starts[None, :]) & (spots[:, None] < ends[None, :])
    return inside.astype(jnp.float32)


def scores(acts, grads, query_in, query_out, lengths):
    groups = lax.axis_size("pb")
    widths = lax.axis_size("wa")
    group = lax.axis_index("pb")
    width_slot = lax.axis_index("wa")
    quarter, half = groups // 4, groups // 2
    tok = acts.shape[0]
    rows = tok // widths
    nseq = lengths.shape[0]
    even = group % 2 == 0

    swap = [(p, p ^ 1) for p in range(groups)]
    ahead = [(p, (p + 2) % groups) for p in range(groups)]
    back = [(p, (p - quarter) % groups) for p in range(groups)]
    flip = [(p, (p - 1 + half) % groups) for p in range(1, groups, 2)]

    side_out = moved(grads, swap)
    last_out = moved(grads, ahead)
    far_out = moved(query_out, back)
    flip_out = moved(grads, flip)
    side_in = moved(acts, swap)
    last_in = moved(acts, ahead)
    far_in = moved(query_in, back)
    flip_in = moved(acts, flip)
    lasts_out = moved(last_out, swap)
    lasts_in = moved(last_in, swap)
    edge_out = jnp.where(even, flip_out, side_out)
    edge_in = jnp.where(even, flip_in, side_in)

    own_in = project(acts, query_in)
    own_out = project(grads, query_out)
    rest_out = [
        project(edge_out, query_out),
        project(last_out, query_out),
        project(lasts_out, query_out),
        project(grads, far_out),
        project(side_out, far_out),
        project(last_out, far_out),
        project(lasts_out, far_out),
    ]
    outs = summed([own_out, *rest_out], widths)
    deep_in = [
        project(edge_in, query_in),
        project(last_in, query_in),
        project(lasts_in, query_in),
        project(acts, far_in),
        project(side_in, far_in),
        project(last_in, far_in),
        project(lasts_in, far_in),
    ]
    ins = summed_narrow([own_in, *deep_in], widths)
    ends = jnp.cumsum(lengths)
    starts = ends - lengths

    def table(block):
        return member_table(starts, ends, block * tok + width_slot * rows, rows)

    here, side = group, group ^ 1
    edge = jnp.where(even, (group + groups - half + 1) % groups, side)
    last, lasts = (group + groups - 2) % groups, (side + groups - 2) % groups
    t_own, t_side, t_edge, t_last, t_lasts = [table(b) for b in (here, side, edge, last, lasts)]

    def totals(proj_in, proj_out, tables):
        products = jnp.concatenate([a * b for a, b in zip(proj_in, proj_out)], axis=0)
        table = jnp.concatenate(tables, axis=0)
        by_rank = lax.dot_general(
            products, table, (((0,), (0,)), ((), ())), precision=lax.Precision.HIGHEST
        )
        return jnp.sum(by_rank.reshape(-1, RANK, nseq), axis=1)

    near_total = totals(ins[:4], outs[:4], [t_own, t_edge, t_last, t_lasts])
    far_total = totals(ins[4:], outs[4:], [t_own, t_side, t_last, t_lasts])
    share = nseq // widths
    both = jnp.concatenate([near_total, far_total], axis=0)
    both = jnp.moveaxis(both.reshape(both.shape[0], widths, share), 1, 0)
    came = jnp.sum(lax.all_to_all(both, "wa", 0, 0, tiled=True), axis=0)
    queries = near_total.shape[0]
    forward = [(p, (p + quarter) % groups) for p in range(groups)]
    mine = came[:queries] + moved(came[queries:], forward)
    lengths_float = lengths.astype(jnp.float32)
    my_lengths = lax.dynamic_slice_in_dim(lengths_float, width_slot * share, share, 0)
    return mine / my_lengths[None, :]


def solution(mesh):
    return jax.shard_map(
        scores,
        mesh=mesh,
        in_specs=(P("pb", "wa"), P("pb", "wa"), P("wa", "pb"), P("wa", "pb"), P()),
        out_specs=P("pb", "wa"),
        check_vma=False,
    )
```

```python
import functools

import jax
import jax.numpy as jnp
from jax import lax
from jax.experimental import pallas as pl
from jax.experimental.pallas import tpu as pltpu
from jax.sharding import PartitionSpec as P


RANK = 32
LANES = 128


def moved(value, pairs):
    return lax.ppermute(value, "pb", pairs)


def fan_kernel(sides, even_ref, flip_ref, *refs):
    token_refs, query_refs, out_ref = refs[:4], refs[4:-1], refs[-1]
    own_ref, side_ref, last_ref, lasts_ref = token_refs

    def put(slot, tokens, queries):
        width = queries.shape[1]
        out_ref[:, slot * width : (slot + 1) * width] = jnp.dot(
            tokens[...], queries[...], preferred_element_type=jnp.float32
        )

    slot = 0
    for side, queries in zip(sides, query_refs):
        put(slot, own_ref, queries)
        if side == "near":
            at = slot + 1

            @pl.when(even_ref[0] == 1)
            def _():
                put(at, flip_ref, queries)

            @pl.when(even_ref[0] == 0)
            def _():
                put(at, side_ref, queries)

        else:
            put(slot + 1, side_ref, queries)
        put(slot + 2, last_ref, queries)
        put(slot + 3, lasts_ref, queries)
        slot += 4


def fan(sides, even, flip, tokens, queries):
    rows, depth = tokens[0].shape
    width = queries[0].shape[1]
    lanes = 4 * len(sides) * width
    vmem = pl.BlockSpec(memory_space=pltpu.VMEM)
    return pl.pallas_call(
        functools.partial(fan_kernel, sides),
        out_shape=jax.ShapeDtypeStruct((rows, lanes), jnp.float32),
        in_specs=[pl.BlockSpec(memory_space=pltpu.SMEM)] + [vmem] * (5 + len(queries)),
        out_specs=vmem,
        compiler_params=pltpu.CompilerParams(vmem_limit_bytes=16 << 20),
        cost_estimate=pl.CostEstimate(
            flops=2 * rows * depth * lanes,
            bytes_accessed=10 * rows * depth + 2 * depth * width + 4 * rows * lanes,
            transcendentals=0,
        ),
    )(even, flip, *tokens, *queries)


def summed(both, widths):
    rows = both.shape[0] // widths
    came = lax.all_to_all(both, "wa", 0, 0, tiled=True)
    return jnp.sum(came.reshape(widths, rows, both.shape[1]), axis=0)


def summed_narrow(parts, widths):
    rows, lanes = parts[0].shape[0] // widths, sum(p.shape[1] for p in parts)
    largest = functools.reduce(jnp.maximum, [jnp.max(jnp.abs(p)) for p in parts])
    power = 13.0 - jnp.ceil(jnp.log2(jnp.maximum(largest, 1e-30)))
    sent = [(p * jnp.exp2(power)).astype(jnp.float16) for p in parts]
    tag = jnp.full((parts[0].shape[0], LANES), power, jnp.float16)
    came = lax.all_to_all(jnp.concatenate([*sent, tag], axis=1), "wa", 0, 0, tiled=True)
    came = came.reshape(widths, rows, lanes + LANES)
    undo = jnp.exp2(-came[:, :, lanes : lanes + 1].astype(jnp.float32))
    return jnp.sum(came[:, :, :lanes].astype(jnp.float32) * undo, axis=0)


def member_table(starts, ends, first, count):
    spots = first + lax.iota(jnp.int32, count)
    inside = (spots[:, None] >= starts[None, :]) & (spots[:, None] < ends[None, :])
    return inside.astype(jnp.float32)


def scores(acts, grads, query_in, query_out, lengths):
    groups = lax.axis_size("pb")
    widths = lax.axis_size("wa")
    group = lax.axis_index("pb")
    width_slot = lax.axis_index("wa")
    quarter, half = groups // 4, groups // 2
    tok = acts.shape[0]
    rows = tok // widths
    nseq = lengths.shape[0]
    even = group % 2 == 0

    swap = [(p, p ^ 1) for p in range(groups)]
    ahead = [(p, (p + 2) % groups) for p in range(groups)]
    back = [(p, (p - quarter) % groups) for p in range(groups)]
    flip = [(p, (p - 1 + half) % groups) for p in range(1, groups, 2)]

    side_out = moved(grads, swap)
    last_out = moved(grads, ahead)
    far_out = moved(query_out, back)
    flip_out = moved(grads, flip)
    side_in = moved(acts, swap)
    last_in = moved(acts, ahead)
    far_in = moved(query_in, back)
    flip_in = moved(acts, flip)
    lasts_out = moved(last_out, swap)
    lasts_in = moved(last_in, swap)
    parity = even.astype(jnp.int32).reshape(1)
    tokens_out = [grads, side_out, last_out, lasts_out]
    tokens_in = [acts, side_in, last_in, lasts_in]
    both_out = fan(("near", "far"), parity, flip_out, tokens_out, [query_out, far_out])
    outs = summed(both_out, widths)
    near_in = fan(("near",), parity, flip_in, tokens_in, [query_in])
    far_side = fan(("far",), parity, flip_in, tokens_in, [far_in])
    ins = summed_narrow([near_in, far_side], widths)
    products = jnp.split(ins * outs, 8, axis=1)
    ends = jnp.cumsum(lengths)
    starts = ends - lengths

    def table(block):
        return member_table(starts, ends, block * tok + width_slot * rows, rows)

    here, side = group, group ^ 1
    edge = jnp.where(even, (group + groups - half + 1) % groups, side)
    last, lasts = (group + groups - 2) % groups, (side + groups - 2) % groups
    t_own, t_side, t_edge, t_last, t_lasts = [table(b) for b in (here, side, edge, last, lasts)]

    def totals(pieces, tables):
        by_rank = lax.dot_general(
            jnp.concatenate(pieces, axis=0),
            jnp.concatenate(tables, axis=0),
            (((0,), (0,)), ((), ())),
            precision=lax.Precision.HIGHEST,
        )
        return jnp.sum(by_rank.reshape(-1, RANK, nseq), axis=1)

    near_total = totals(products[:4], [t_own, t_edge, t_last, t_lasts])
    far_total = totals(products[4:], [t_own, t_side, t_last, t_lasts])
    share = nseq // widths
    both = jnp.concatenate([near_total, far_total], axis=0)
    both = jnp.moveaxis(both.reshape(both.shape[0], widths, share), 1, 0)
    came = jnp.sum(lax.all_to_all(both, "wa", 0, 0, tiled=True), axis=0)
    queries = near_total.shape[0]
    forward = [(p, (p + quarter) % groups) for p in range(groups)]
    mine = came[:queries] + moved(came[queries:], forward)
    lengths_float = lengths.astype(jnp.float32)
    my_lengths = lax.dynamic_slice_in_dim(lengths_float, width_slot * share, share, 0)
    return mine / my_lengths[None, :]


def solution(mesh):
    return jax.shard_map(
        scores,
        mesh=mesh,
        in_specs=(P("pb", "wa"), P("pb", "wa"), P("wa", "pb"), P("wa", "pb"), P()),
        out_specs=P("pb", "wa"),
        check_vma=False,
    )
```

```python
import functools

import jax
import jax.numpy as jnp
from jax import lax
from jax.experimental import pallas as pl
from jax.experimental.pallas import tpu as pltpu
from jax.sharding import PartitionSpec as P


RANK = 32
LANES = 128
LARGEST = 32000.0
WIDTH = 256


def moved(value, pairs):
    return lax.ppermute(value, "pb", pairs)


def fan_kernel(sides, even_ref, flip_ref, *refs):
    token_refs, query_refs, out_ref = refs[:4], refs[4:-1], refs[-1]
    own_ref, side_ref, last_ref, lasts_ref = token_refs

    rows, tags = out_ref.shape[0], out_ref.shape[1] - LANES
    lane = lax.broadcasted_iota(jnp.int32, (rows, LANES), 1)

    def put(slot, tokens, queries):
        width = queries.shape[1]
        part = jnp.dot(tokens[...], queries[...], preferred_element_type=jnp.float32)
        largest = jnp.maximum(jnp.max(jnp.abs(part), axis=1, keepdims=True), 1e-25)
        power = jnp.floor(jnp.log2(LARGEST / largest))
        coded = jnp.round(part * jnp.exp2(power)).astype(jnp.int32)
        out_ref[:, slot * width : (slot + 1) * width] = coded.astype(jnp.int16)
        held = out_ref[:, tags:].astype(jnp.int32)
        tag = jnp.where(lane == slot, power.astype(jnp.int32), held)
        out_ref[:, tags:] = tag.astype(jnp.int16)

    out_ref[:, tags:] = jnp.zeros((rows, LANES), jnp.int16)

    slot = 0
    for side, queries in zip(sides, query_refs):
        put(slot, own_ref, queries)
        if side == "near":
            at = slot + 1

            @pl.when(even_ref[0] == 1)
            def _():
                put(at, flip_ref, queries)

            @pl.when(even_ref[0] == 0)
            def _():
                put(at, side_ref, queries)

        else:
            put(slot + 1, side_ref, queries)
        put(slot + 2, last_ref, queries)
        put(slot + 3, lasts_ref, queries)
        slot += 4


def fan(sides, even, flip, tokens, queries):
    rows, depth = tokens[0].shape
    width = queries[0].shape[1]
    lanes = 4 * len(sides) * width
    vmem = pl.BlockSpec(memory_space=pltpu.VMEM)
    return pl.pallas_call(
        functools.partial(fan_kernel, sides),
        out_shape=jax.ShapeDtypeStruct((rows, lanes + LANES), jnp.int16),
        in_specs=[pl.BlockSpec(memory_space=pltpu.SMEM)] + [vmem] * (5 + len(queries)),
        out_specs=vmem,
        compiler_params=pltpu.CompilerParams(vmem_limit_bytes=16 << 20),
        cost_estimate=pl.CostEstimate(
            flops=2 * rows * depth * lanes,
            bytes_accessed=10 * rows * depth + 2 * depth * width + 2 * rows * lanes,
            transcendentals=0,
        ),
    )(even, flip, *tokens, *queries)


def summed(coded, widths):
    rows = coded[0].shape[0] // widths
    both = jnp.concatenate(coded, axis=1) if len(coded) > 1 else coded[0]
    came = lax.all_to_all(both, "wa", 0, 0, tiled=True)
    came = came.reshape(widths, rows, both.shape[1])
    pieces, at = [], 0
    for part in coded:
        tags = part.shape[1] - LANES
        slots = tags // WIDTH
        powers = came[:, :, at + tags : at + tags + slots].astype(jnp.float32)
        undo = jnp.exp2(-powers)
        for slot in range(slots):
            values = came[:, :, at + slot * WIDTH : at + (slot + 1) * WIDTH]
            scale = undo[:, :, slot : slot + 1]
            pieces.append(jnp.sum(values.astype(jnp.float32) * scale, axis=0))
        at += part.shape[1]
    return pieces


def member_table(starts, ends, first, count):
    spots = first + lax.iota(jnp.int32, count)
    inside = (spots[:, None] >= starts[None, :]) & (spots[:, None] < ends[None, :])
    return inside.astype(jnp.float32)


def scores(acts, grads, query_in, query_out, lengths):
    groups = lax.axis_size("pb")
    widths = lax.axis_size("wa")
    group = lax.axis_index("pb")
    width_slot = lax.axis_index("wa")
    quarter, half = groups // 4, groups // 2
    tok = acts.shape[0]
    rows = tok // widths
    nseq = lengths.shape[0]
    even = group % 2 == 0

    swap = [(p, p ^ 1) for p in range(groups)]
    ahead = [(p, (p + 2) % groups) for p in range(groups)]
    back = [(p, (p - quarter) % groups) for p in range(groups)]
    flip = [(p, (p - 1 + half) % groups) for p in range(1, groups, 2)]

    side_out = moved(grads, swap)
    last_out = moved(grads, ahead)
    far_out = moved(query_out, back)
    flip_out = moved(grads, flip)
    side_in = moved(acts, swap)
    last_in = moved(acts, ahead)
    far_in = moved(query_in, back)
    flip_in = moved(acts, flip)
    lasts_out = moved(last_out, swap)
    lasts_in = moved(last_in, swap)
    parity = even.astype(jnp.int32).reshape(1)
    tokens_out = [grads, side_out, last_out, lasts_out]
    tokens_in = [acts, side_in, last_in, lasts_in]
    both_out = fan(("near", "far"), parity, flip_out, tokens_out, [query_out, far_out])
    outs = summed([both_out], widths)
    near_in = fan(("near",), parity, flip_in, tokens_in, [query_in])
    far_side = fan(("far",), parity, flip_in, tokens_in, [far_in])
    ins = summed([near_in, far_side], widths)
    products = [a * b for a, b in zip(ins, outs)]
    ends = jnp.cumsum(lengths)
    starts = ends - lengths

    def table(block):
        return member_table(starts, ends, block * tok + width_slot * rows, rows)

    here, side = group, group ^ 1
    edge = jnp.where(even, (group + groups - half + 1) % groups, side)
    last, lasts = (group + groups - 2) % groups, (side + groups - 2) % groups
    t_own, t_side, t_edge, t_last, t_lasts = [table(b) for b in (here, side, edge, last, lasts)]

    def totals(pieces, tables):
        by_rank = lax.dot_general(
            jnp.concatenate(pieces, axis=0),
            jnp.concatenate(tables, axis=0),
            (((0,), (0,)), ((), ())),
            precision=lax.Precision.HIGHEST,
        )
        return jnp.sum(by_rank.reshape(-1, RANK, nseq), axis=1)

    near_total = totals(products[:4], [t_own, t_edge, t_last, t_lasts])
    far_total = totals(products[4:], [t_own, t_side, t_last, t_lasts])
    share = nseq // widths
    both = jnp.concatenate([near_total, far_total], axis=0)
    both = jnp.moveaxis(both.reshape(both.shape[0], widths, share), 1, 0)
    came = jnp.sum(lax.all_to_all(both, "wa", 0, 0, tiled=True), axis=0)
    queries = near_total.shape[0]
    forward = [(p, (p + quarter) % groups) for p in range(groups)]
    mine = came[:queries] + moved(came[queries:], forward)
    lengths_float = lengths.astype(jnp.float32)
    my_lengths = lax.dynamic_slice_in_dim(lengths_float, width_slot * share, share, 0)
    return mine / my_lengths[None, :]


def solution(mesh):
    return jax.shard_map(
        scores,
        mesh=mesh,
        in_specs=(P("pb", "wa"), P("pb", "wa"), P("wa", "pb"), P("wa", "pb"), P()),
        out_specs=P("pb", "wa"),
        check_vma=False,
    )
```

```python
import jax
import jax.numpy as jnp
from jax import lax
from jax.experimental import pallas as pl
from jax.experimental.pallas import tpu as pltpu
from jax.sharding import PartitionSpec as P


RANK = 32
LANES = 128
LARGEST = 32000.0
WIDTH = 256


def moved(value, pairs):
    return lax.ppermute(value, "pb", pairs)


def code(part, slot, out_ref):
    width, rows, tags = part.shape[1], out_ref.shape[0], out_ref.shape[1] - LANES
    lane = lax.broadcasted_iota(jnp.int32, (rows, LANES), 1)
    largest = jnp.maximum(jnp.max(jnp.abs(part), axis=1, keepdims=True), 1e-25)
    power = jnp.floor(jnp.log2(LARGEST / largest))
    coded = jnp.round(part * jnp.exp2(power)).astype(jnp.int32)
    out_ref[:, slot * width : (slot + 1) * width] = coded.astype(jnp.int16)
    held = out_ref[:, tags:].astype(jnp.int32)
    tag = jnp.where(lane == slot, power.astype(jnp.int32), held)
    out_ref[:, tags:] = tag.astype(jnp.int16)


def put(slot, tokens, queries, out_ref):
    part = jnp.dot(tokens[...], queries[...], preferred_element_type=jnp.float32)
    code(part, slot, out_ref)


def near_rows(even_ref, own, side, flip, last, lasts, queries, out_ref):
    out_ref[:, out_ref.shape[1] - LANES :] = jnp.zeros((out_ref.shape[0], LANES), jnp.int16)
    put(0, own, queries, out_ref)

    @pl.when(even_ref[0] == 1)
    def _():
        put(1, flip, queries, out_ref)

    @pl.when(even_ref[0] == 0)
    def _():
        put(1, side, queries, out_ref)

    put(2, last, queries, out_ref)
    put(3, lasts, queries, out_ref)


def far_rows(own, side, last, lasts, queries, out_ref):
    put(4, own, queries, out_ref)
    put(5, side, queries, out_ref)
    put(6, last, queries, out_ref)
    put(7, lasts, queries, out_ref)


def rest_kernel(even, own, side, flip, last, lasts, near, far, out_ref):
    near_rows(even, own, side, flip, last, lasts, near, out_ref)
    far_rows(own, side, last, lasts, far, out_ref)


def near_kernel(even, own, side, flip, last, lasts, near, out_ref):
    near_rows(even, own, side, flip, last, lasts, near, out_ref)


def far_kernel(odd_ref, own, side, last, lasts, whole, top, bottom, begun, out_ref, far):
    half, lanes = top.shape[0], begun.shape[1] - LANES

    @pl.when(odd_ref[0] == 1)
    def _():
        far[...] = whole[...]

    @pl.when(odd_ref[0] == 0)
    def _():
        far[:half, :] = top[...]
        far[half:, :] = bottom[...]

    out_ref[:, :lanes] = begun[:, :lanes]
    out_ref[:, out_ref.shape[1] - LANES :] = begun[:, lanes:]
    far_rows(own, side, last, lasts, far, out_ref)


def call(kernel, slots, scalar, arrays, scratch=()):
    rows, depth = arrays[0].shape
    lanes = slots * WIDTH
    vmem = pl.BlockSpec(memory_space=pltpu.VMEM)
    return pl.pallas_call(
        kernel,
        out_shape=jax.ShapeDtypeStruct((rows, lanes + LANES), jnp.int16),
        in_specs=[pl.BlockSpec(memory_space=pltpu.SMEM)] + [vmem] * len(arrays),
        out_specs=vmem,
        scratch_shapes=list(scratch),
        compiler_params=pltpu.CompilerParams(vmem_limit_bytes=16 << 20),
        cost_estimate=pl.CostEstimate(
            flops=2 * rows * depth * lanes,
            bytes_accessed=sum(a.size for a in arrays) * 2 + 2 * rows * lanes,
            transcendentals=0,
        ),
    )(scalar, *arrays)


def summed(coded, widths):
    rows = coded.shape[0] // widths
    came = lax.all_to_all(coded, "wa", 0, 0, tiled=True)
    came = came.reshape(widths, rows, coded.shape[1])
    tags = coded.shape[1] - LANES
    slots = tags // WIDTH
    undo = jnp.exp2(-came[:, :, tags : tags + slots].astype(jnp.float32))
    pieces = []
    for slot in range(slots):
        values = came[:, :, slot * WIDTH : (slot + 1) * WIDTH]
        scale = undo[:, :, slot : slot + 1]
        pieces.append(jnp.sum(values.astype(jnp.float32) * scale, axis=0))
    return pieces


def member_table(starts, ends, first, count):
    spots = first + lax.iota(jnp.int32, count)
    inside = (spots[:, None] >= starts[None, :]) & (spots[:, None] < ends[None, :])
    return inside.astype(jnp.float32)


def scores(acts, grads, query_in, query_out, lengths):
    groups = lax.axis_size("pb")
    widths = lax.axis_size("wa")
    group = lax.axis_index("pb")
    width_slot = lax.axis_index("wa")
    quarter, half = groups // 4, groups // 2
    tok = acts.shape[0]
    rows = tok // widths
    nseq = lengths.shape[0]
    even = group % 2 == 0

    swap = [(p, p ^ 1) for p in range(groups)]
    ahead = [(p, (p + 2) % groups) for p in range(groups)]
    back = [(p, (p - quarter) % groups) for p in range(groups)]
    flip = [(p, (p - 1 + half) % groups) for p in range(1, groups, 2)]

    side_out = moved(grads, swap)
    last_out = moved(grads, ahead)
    far_out = moved(query_out, back)
    flip_out = moved(grads, flip)
    odd_chips = [p for p in range(groups) if p // 2 % 2 == 1]
    even_chips = [p for p in range(groups) if p // 2 % 2 == 0]
    cut = query_in.shape[0] // 2
    top, bottom = query_in[:cut], query_in[cut:]
    hop = moved(bottom, [(p, (p - 2) % groups) for p in even_chips])
    far_whole = moved(query_in, [(p, (p - quarter) % groups) for p in odd_chips])
    side_in = moved(acts, swap)
    last_in = moved(acts, ahead)
    far_top = moved(top, [(p, (p - quarter) % groups) for p in even_chips])
    flip_in = moved(acts, flip)
    far_bottom = moved(hop, [(p, (p - 2) % groups) for p in odd_chips])
    lasts_out = moved(last_out, swap)
    lasts_in = moved(last_in, swap)
    parity = even.astype(jnp.int32).reshape(1)
    odd_chip = (group // 2 % 2).astype(jnp.int32).reshape(1)
    coded_out = call(
        rest_kernel, 8, parity, [grads, side_out, flip_out, last_out, lasts_out, query_out, far_out]
    )
    outs = summed(coded_out, widths)
    near_in = call(near_kernel, 4, parity, [acts, side_in, flip_in, last_in, lasts_in, query_in])
    coded_in = call(
        far_kernel,
        8,
        odd_chip,
        [acts, side_in, last_in, lasts_in, far_whole, far_top, far_bottom, near_in],
        [pltpu.VMEM(query_in.shape, query_in.dtype)],
    )
    ins = summed(coded_in, widths)
    products = [a * b for a, b in zip(ins, outs)]
    ends = jnp.cumsum(lengths)
    starts = ends - lengths

    def table(block):
        return member_table(starts, ends, block * tok + width_slot * rows, rows)

    here, side = group, group ^ 1
    edge = jnp.where(even, (group + groups - half + 1) % groups, side)
    last, lasts = (group + groups - 2) % groups, (side + groups - 2) % groups
    t_own, t_side, t_edge, t_last, t_lasts = [table(b) for b in (here, side, edge, last, lasts)]

    def totals(pieces, tables):
        by_rank = lax.dot_general(
            jnp.concatenate(pieces, axis=0),
            jnp.concatenate(tables, axis=0),
            (((0,), (0,)), ((), ())),
            precision=lax.Precision.HIGHEST,
        )
        return jnp.sum(by_rank.reshape(-1, RANK, nseq), axis=1)

    near_total = totals(products[:4], [t_own, t_edge, t_last, t_lasts])
    far_total = totals(products[4:], [t_own, t_side, t_last, t_lasts])
    share = nseq // widths
    both = jnp.concatenate([near_total, far_total], axis=0)
    both = jnp.moveaxis(both.reshape(both.shape[0], widths, share), 1, 0)
    came = jnp.sum(lax.all_to_all(both, "wa", 0, 0, tiled=True), axis=0)
    queries = near_total.shape[0]
    forward = [(p, (p + quarter) % groups) for p in range(groups)]
    mine = came[:queries] + moved(came[queries:], forward)
    lengths_float = lengths.astype(jnp.float32)
    my_lengths = lax.dynamic_slice_in_dim(lengths_float, width_slot * share, share, 0)
    return mine / my_lengths[None, :]


def solution(mesh):
    return jax.shard_map(
        scores,
        mesh=mesh,
        in_specs=(P("pb", "wa"), P("pb", "wa"), P("wa", "pb"), P("wa", "pb"), P()),
        out_specs=P("pb", "wa"),
        check_vma=False,
    )
```

```python
import functools

import jax
import jax.numpy as jnp
from jax import lax
from jax.experimental import pallas as pl
from jax.experimental.pallas import tpu as pltpu
from jax.sharding import PartitionSpec as P


RANK = 32
LANES = 128
LARGEST = 32000.0
WIDTH = 256


def moved(value, pairs):
    return lax.ppermute(value, "pb", pairs)


def code(part, slot, out_ref):
    width, rows, tags = part.shape[1], out_ref.shape[0], out_ref.shape[1] - LANES
    lane = lax.broadcasted_iota(jnp.int32, (rows, LANES), 1)
    largest = jnp.maximum(jnp.max(jnp.abs(part), axis=1, keepdims=True), 1e-25)
    power = jnp.floor(jnp.log2(LARGEST / largest))
    coded = jnp.round(part * jnp.exp2(power)).astype(jnp.int32)
    out_ref[:, slot * width : (slot + 1) * width] = coded.astype(jnp.int16)
    held = out_ref[:, tags:].astype(jnp.int32)
    tag = jnp.where(lane == slot, power.astype(jnp.int32), held)
    out_ref[:, tags:] = tag.astype(jnp.int16)


def put(slot, tokens, queries, out_ref):
    part = jnp.dot(tokens[...], queries[...], preferred_element_type=jnp.float32)
    code(part, slot, out_ref)


def near_rows(even_ref, own, side, flip, last, lasts, queries, out_ref):
    out_ref[:, out_ref.shape[1] - LANES :] = jnp.zeros((out_ref.shape[0], LANES), jnp.int16)
    put(0, own, queries, out_ref)

    @pl.when(even_ref[0] == 1)
    def _():
        put(1, flip, queries, out_ref)

    @pl.when(even_ref[0] == 0)
    def _():
        put(1, side, queries, out_ref)

    put(2, last, queries, out_ref)
    put(3, lasts, queries, out_ref)


def far_rows(own, side, last, lasts, queries, out_ref):
    put(4, own, queries, out_ref)
    put(5, side, queries, out_ref)
    put(6, last, queries, out_ref)
    put(7, lasts, queries, out_ref)


def rest_kernel(even, own, side, flip, last, lasts, near, far, out_ref):
    near_rows(even, own, side, flip, last, lasts, near, out_ref)
    far_rows(own, side, last, lasts, far, out_ref)


def near_kernel(even, own, side, flip, last, lasts, near, out_ref):
    near_rows(even, own, side, flip, last, lasts, near, out_ref)


def far_kernel(even, own, side, last, lasts, far, begun, out_ref):
    lanes = begun.shape[1] - LANES
    out_ref[:, :lanes] = begun[:, :lanes]
    out_ref[:, out_ref.shape[1] - LANES :] = begun[:, lanes:]
    far_rows(own, side, last, lasts, far, out_ref)


def decoded(came_ref, rows):
    lanes = came_ref.shape[1] - LANES
    undo = jnp.exp2(-came_ref[:, lanes:].astype(jnp.int32).astype(jnp.float32))
    pieces = []
    for slot in range(lanes // WIDTH):
        total = jnp.zeros((rows, WIDTH), jnp.float32)
        for at in range(0, came_ref.shape[0], rows):
            values = came_ref[at : at + rows, slot * WIDTH : (slot + 1) * WIDTH]
            scale = undo[at : at + rows, slot : slot + 1]
            total = total + values.astype(jnp.int32).astype(jnp.float32) * scale
        pieces.append(total)
    return pieces


def open_kernel(rows, came_ref, out_ref):
    for slot, piece in enumerate(decoded(came_ref, rows)):
        out_ref[slot * rows : (slot + 1) * rows, :] = piece


def close_kernel(rows, came_ref, outs_ref, near_ref, far_ref, out_ref):
    products = [
        piece * outs_ref[slot * rows : (slot + 1) * rows, :]
        for slot, piece in enumerate(decoded(came_ref, rows))
    ]
    half, queries = len(products) // 2, WIDTH // RANK
    for at, (group, table) in enumerate(
        [(products[:half], near_ref), (products[half:], far_ref)]
    ):
        by_rank = lax.dot_general(
            jnp.concatenate(group, axis=0),
            table[...],
            (((0,), (0,)), ((), ())),
            precision=lax.Precision.HIGHEST,
            preferred_element_type=jnp.float32,
        )
        total = jnp.sum(by_rank.reshape(queries, RANK, by_rank.shape[1]), axis=1)
        out_ref[at * queries : (at + 1) * queries, :] = total


def small(kernel, shape, arrays):
    return pl.pallas_call(
        kernel,
        out_shape=jax.ShapeDtypeStruct(shape, jnp.float32),
        compiler_params=pltpu.CompilerParams(vmem_limit_bytes=16 << 20),
        cost_estimate=pl.CostEstimate(
            flops=4 * arrays[0].size, bytes_accessed=2 * arrays[0].size, transcendentals=0
        ),
    )(*arrays)


def call(kernel, slots, scalar, arrays, scratch=()):
    rows, depth = arrays[0].shape
    lanes = slots * WIDTH
    vmem = pl.BlockSpec(memory_space=pltpu.VMEM)
    return pl.pallas_call(
        kernel,
        out_shape=jax.ShapeDtypeStruct((rows, lanes + LANES), jnp.int16),
        in_specs=[pl.BlockSpec(memory_space=pltpu.SMEM)] + [vmem] * len(arrays),
        out_specs=vmem,
        scratch_shapes=list(scratch),
        compiler_params=pltpu.CompilerParams(vmem_limit_bytes=16 << 20),
        cost_estimate=pl.CostEstimate(
            flops=2 * rows * depth * lanes,
            bytes_accessed=sum(a.size for a in arrays) * 2 + 2 * rows * lanes,
            transcendentals=0,
        ),
    )(scalar, *arrays)


def exchanged(coded):
    return lax.all_to_all(coded, "wa", 0, 0, tiled=True)


def member_table(starts, ends, first, count):
    spots = first + lax.iota(jnp.int32, count)
    inside = (spots[:, None] >= starts[None, :]) & (spots[:, None] < ends[None, :])
    return inside.astype(jnp.float32)


def scores(acts, grads, query_in, query_out, lengths):
    groups = lax.axis_size("pb")
    widths = lax.axis_size("wa")
    group = lax.axis_index("pb")
    width_slot = lax.axis_index("wa")
    quarter, half = groups // 4, groups // 2
    tok = acts.shape[0]
    rows = tok // widths
    nseq = lengths.shape[0]
    even = group % 2 == 0

    swap = [(p, p ^ 1) for p in range(groups)]
    ahead = [(p, (p + 2) % groups) for p in range(groups)]
    back = [(p, (p - quarter) % groups) for p in range(groups)]
    flip = [(p, (p - 1 + half) % groups) for p in range(1, groups, 2)]

    side_out = moved(grads, swap)
    last_out = moved(grads, ahead)
    far_out = moved(query_out, back)
    flip_out = moved(grads, flip)
    last_in = moved(acts, ahead)
    far_in = moved(query_in, back)
    flip_in = moved(acts, flip)
    side_in = moved(acts, swap)
    lasts_out = moved(last_out, swap)
    lasts_in = moved(last_in, swap)
    parity = even.astype(jnp.int32).reshape(1)
    coded_out = call(
        rest_kernel, 8, parity, [grads, side_out, flip_out, last_out, lasts_out, query_out, far_out]
    )
    came_out = exchanged(coded_out)
    outs = small(functools.partial(open_kernel, rows), (8 * rows, WIDTH), [came_out])
    near_in = call(near_kernel, 4, parity, [acts, side_in, flip_in, last_in, lasts_in, query_in])
    coded_in = call(far_kernel, 8, parity, [acts, side_in, last_in, lasts_in, far_in, near_in])
    came_in = exchanged(coded_in)
    ends = jnp.cumsum(lengths)
    starts = ends - lengths

    def table(block):
        return member_table(starts, ends, block * tok + width_slot * rows, rows)

    here, side = group, group ^ 1
    edge = jnp.where(even, (group + groups - half + 1) % groups, side)
    last, lasts = (group + groups - 2) % groups, (side + groups - 2) % groups
    t_own, t_side, t_edge, t_last, t_lasts = [table(b) for b in (here, side, edge, last, lasts)]

    near_table = jnp.concatenate([t_own, t_edge, t_last, t_lasts], axis=0)
    far_table = jnp.concatenate([t_own, t_side, t_last, t_lasts], axis=0)
    queries = query_in.shape[1] // RANK
    both = small(
        functools.partial(close_kernel, rows),
        (2 * queries, nseq),
        [came_in, outs, near_table, far_table],
    )
    share = nseq // widths
    both = jnp.moveaxis(both.reshape(both.shape[0], widths, share), 1, 0)
    came = jnp.sum(lax.all_to_all(both, "wa", 0, 0, tiled=True), axis=0)
    forward = [(p, (p + quarter) % groups) for p in range(groups)]
    mine = came[:queries] + moved(came[queries:], forward)
    lengths_float = lengths.astype(jnp.float32)
    my_lengths = lax.dynamic_slice_in_dim(lengths_float, width_slot * share, share, 0)
    return mine / my_lengths[None, :]


def solution(mesh):
    return jax.shard_map(
        scores,
        mesh=mesh,
        in_specs=(P("pb", "wa"), P("pb", "wa"), P("wa", "pb"), P("wa", "pb"), P()),
        out_specs=P("pb", "wa"),
        check_vma=False,
    )
```

```python
import functools

import jax
import jax.numpy as jnp
from jax import lax
from jax.experimental import pallas as pl
from jax.experimental.pallas import tpu as pltpu
from jax.sharding import PartitionSpec as P


RANK = 32
LANES = 128
LARGEST = 32000.0
WIDTH = 256


def moved(value, pairs):
    return lax.ppermute(value, "pb", pairs)


def code(part, slot, out_ref):
    width, rows, tags = part.shape[1], out_ref.shape[0], out_ref.shape[1] - LANES
    lane = lax.broadcasted_iota(jnp.int32, (rows, LANES), 1)
    largest = jnp.maximum(jnp.max(jnp.abs(part), axis=1, keepdims=True), 1e-25)
    power = jnp.floor(jnp.log2(LARGEST / largest))
    coded = jnp.round(part * jnp.exp2(power)).astype(jnp.int32)
    out_ref[:, slot * width : (slot + 1) * width] = coded.astype(jnp.int16)
    held = out_ref[:, tags:].astype(jnp.int32)
    tag = jnp.where(lane == slot, power.astype(jnp.int32), held)
    out_ref[:, tags:] = tag.astype(jnp.int16)


def put(slot, tokens, queries, out_ref):
    part = jnp.dot(tokens[...], queries[...], preferred_element_type=jnp.float32)
    code(part, slot, out_ref)


def near_rows(even_ref, own, side, flip, last, lasts, queries, out_ref):
    out_ref[:, out_ref.shape[1] - LANES :] = jnp.zeros((out_ref.shape[0], LANES), jnp.int16)
    put(0, own, queries, out_ref)

    @pl.when(even_ref[0] == 1)
    def _():
        put(1, flip, queries, out_ref)

    @pl.when(even_ref[0] == 0)
    def _():
        put(1, side, queries, out_ref)

    put(2, last, queries, out_ref)
    put(3, lasts, queries, out_ref)


def far_rows(own, side, last, lasts, queries, out_ref):
    put(4, own, queries, out_ref)
    put(5, side, queries, out_ref)
    put(6, last, queries, out_ref)
    put(7, lasts, queries, out_ref)


def rest_kernel(even, own, side, flip, last, lasts, near, far, out_ref):
    near_rows(even, own, side, flip, last, lasts, near, out_ref)
    far_rows(own, side, last, lasts, far, out_ref)


def near_kernel(even, own, side, flip, last, lasts, near, out_ref):
    near_rows(even, own, side, flip, last, lasts, near, out_ref)


def far_kernel(even, own, side, last, lasts, far, begun, out_ref):
    lanes = begun.shape[1] - LANES
    out_ref[:, :lanes] = begun[:, :lanes]
    out_ref[:, out_ref.shape[1] - LANES :] = begun[:, lanes:]
    far_rows(own, side, last, lasts, far, out_ref)


def decoded(came_ref, rows):
    lanes = came_ref.shape[1] - LANES
    undo = jnp.exp2(-came_ref[:, lanes:].astype(jnp.int32).astype(jnp.float32))
    pieces = []
    for slot in range(lanes // WIDTH):
        total = jnp.zeros((rows, WIDTH), jnp.float32)
        for at in range(0, came_ref.shape[0], rows):
            values = came_ref[at : at + rows, slot * WIDTH : (slot + 1) * WIDTH]
            scale = undo[at : at + rows, slot : slot + 1]
            total = total + values.astype(jnp.int32).astype(jnp.float32) * scale
        pieces.append(total)
    return pieces


def open_kernel(rows, came_ref, out_ref):
    for slot, piece in enumerate(decoded(came_ref, rows)):
        out_ref[slot * rows : (slot + 1) * rows, :] = piece


def close_kernel(rows, came_ref, outs_ref, near_ref, far_ref, out_ref):
    products = [
        piece * outs_ref[slot * rows : (slot + 1) * rows, :]
        for slot, piece in enumerate(decoded(came_ref, rows))
    ]
    half, queries = len(products) // 2, WIDTH // RANK
    for at, (group, table) in enumerate(
        [(products[:half], near_ref), (products[half:], far_ref)]
    ):
        by_rank = lax.dot_general(
            jnp.concatenate(group, axis=0),
            table[...],
            (((0,), (0,)), ((), ())),
            precision=lax.Precision.HIGHEST,
            preferred_element_type=jnp.float32,
        )
        total = jnp.sum(by_rank.reshape(queries, RANK, by_rank.shape[1]), axis=1)
        out_ref[at * queries : (at + 1) * queries, :] = total


def small(kernel, shape, arrays):
    return pl.pallas_call(
        kernel,
        out_shape=jax.ShapeDtypeStruct(shape, jnp.float32),
        compiler_params=pltpu.CompilerParams(vmem_limit_bytes=16 << 20),
        cost_estimate=pl.CostEstimate(
            flops=4 * arrays[0].size, bytes_accessed=2 * arrays[0].size, transcendentals=0
        ),
    )(*arrays)


def call(kernel, slots, scalar, arrays, scratch=()):
    rows, depth = arrays[0].shape
    lanes = slots * WIDTH
    vmem = pl.BlockSpec(memory_space=pltpu.VMEM)
    return pl.pallas_call(
        kernel,
        out_shape=jax.ShapeDtypeStruct((rows, lanes + LANES), jnp.int16),
        in_specs=[pl.BlockSpec(memory_space=pltpu.SMEM)] + [vmem] * len(arrays),
        out_specs=vmem,
        scratch_shapes=list(scratch),
        compiler_params=pltpu.CompilerParams(vmem_limit_bytes=16 << 20),
        cost_estimate=pl.CostEstimate(
            flops=2 * rows * depth * lanes,
            bytes_accessed=sum(a.size for a in arrays) * 2 + 2 * rows * lanes,
            transcendentals=0,
        ),
    )(scalar, *arrays)


def exchanged(coded):
    return lax.all_to_all(coded, "wa", 0, 0, tiled=True)


def member_table(starts, ends, first, count):
    spots = first + lax.iota(jnp.int32, count)
    inside = (spots[:, None] >= starts[None, :]) & (spots[:, None] < ends[None, :])
    return inside.astype(jnp.float32)


def scores(acts, grads, query_in, query_out, lengths):
    groups = lax.axis_size("pb")
    widths = lax.axis_size("wa")
    group = lax.axis_index("pb")
    width_slot = lax.axis_index("wa")
    quarter, half = groups // 4, groups // 2
    tok = acts.shape[0]
    rows = tok // widths
    nseq = lengths.shape[0]
    even = group % 2 == 0

    swap = [(p, p ^ 1) for p in range(groups)]
    ahead = [(p, (p + 2) % groups) for p in range(groups)]
    back = [(p, (p - quarter) % groups) for p in range(groups)]
    flip = [(p, (p - 1 + half) % groups) for p in range(1, groups, 2)]

    side_out = moved(grads, swap)
    last_out = moved(grads, ahead)
    far_out = moved(query_out, back)
    flip_out = moved(grads, flip)
    last_in = moved(acts, ahead)
    far_in = moved(query_in, back)
    flip_in = moved(acts, flip)
    side_in = moved(acts, swap)
    lasts_out = moved(last_out, swap)
    lasts_in = moved(last_in, swap)
    parity = even.astype(jnp.int32).reshape(1)
    coded_out = call(
        rest_kernel, 8, parity, [grads, side_out, flip_out, last_out, lasts_out, query_out, far_out]
    )
    came_out = exchanged(coded_out)
    outs = small(functools.partial(open_kernel, rows), (8 * rows, WIDTH), [came_out])
    near_in = call(near_kernel, 4, parity, [acts, side_in, flip_in, last_in, lasts_in, query_in])
    coded_in = call(far_kernel, 8, parity, [acts, side_in, last_in, lasts_in, far_in, near_in])
    came_in = exchanged(coded_in)
    ends = jnp.cumsum(lengths)
    starts = ends - lengths

    def table(block):
        return member_table(starts, ends, block * tok + width_slot * rows, rows)

    here, side = group, group ^ 1
    edge = jnp.where(even, (group + groups - half + 1) % groups, side)
    last, lasts = (group + groups - 2) % groups, (side + groups - 2) % groups
    t_own, t_side, t_edge, t_last, t_lasts = [table(b) for b in (here, side, edge, last, lasts)]

    near_table = jnp.concatenate([t_own, t_edge, t_last, t_lasts], axis=0)
    far_table = jnp.concatenate([t_own, t_side, t_last, t_lasts], axis=0)
    queries = query_in.shape[1] // RANK
    both = small(
        functools.partial(close_kernel, rows),
        (2 * queries, nseq),
        [came_in, outs, near_table, far_table],
    )
    share = nseq // widths
    forward = [(p, (p + quarter) % groups) for p in range(groups)]
    total = both[:queries] + moved(both[queries:], forward)
    total = jnp.moveaxis(total.reshape(queries, widths, share), 1, 0)
    mine = jnp.sum(lax.all_to_all(total, "wa", 0, 0, tiled=True), axis=0)
    lengths_float = lengths.astype(jnp.float32)
    my_lengths = lax.dynamic_slice_in_dim(lengths_float, width_slot * share, share, 0)
    return mine / my_lengths[None, :]


def solution(mesh):
    return jax.shard_map(
        scores,
        mesh=mesh,
        in_specs=(P("pb", "wa"), P("pb", "wa"), P("wa", "pb"), P("wa", "pb"), P()),
        out_specs=P("pb", "wa"),
        check_vma=False,
    )
```
